32 devices in a mesh: group: 8 (over z, x), local: 4 (over y, core).
Axes of the slice: x: 2, y: 2, z: 4, core: 2. Of those that a mesh axis runs over, the one named last changes fastest.
Arguments:
- ids: int32 [4096, 32, 8], P(('group', 'local')), may hold values from 0 to 4095
- lengths: int32 [4096, 32], P(('group', 'local')), may hold values from 1 to 8, as said below
- id_weights: float32 [4096, 32, 8], P(('group', 'local')), may hold values from 0.5 to 1.5
- table: float32 [131072, 256], P(('group', 'local')), may hold values from -2.4 to 2.4
Outputs:
- pooled: float32 [4096, 32, 256], P(('group', 'local'))
The draws below stay inside these ranges and needn't reach their ends.
Inputs may be any that keep to these rules, and one draw needn't show every extreme that they name: `lengths`: every draw has some bag with 8 live ids.
All inputs are finite; a program needn't handle non-finite values.
Results may differ from the reference program's by a relative error of at most 0.00002.
Values sent between devices are 32-bit elements; how exact they have to be, the bound alone decides.
No kernel may reach another device: no remote copies, remote signals or barrier semaphores. Data moves between devices by JAX's collectives and lax.ppermute only.
A program may use at most 128 MiB of HBM per device.

```python
import math
import jax
import jax.numpy as jnp
import numpy as np
from jax import lax

DIM = 256
BAG = 8
EX_DEV = 128
ROWS = 4096
TABLES = 32
EXAMPLES = 4096
DEVICES = 32


def draw_lengths(key, part):
    first, second, third, fourth = jax.random.split(jax.random.fold_in(key, 17), 4)
    limits = jax.random.randint(first, (TABLES,), BAG // 2, BAG + 1)
    busiest = jax.random.randint(second, (), 0, TABLES)
    columns = jnp.arange(TABLES)
    limits = jnp.where(columns == busiest, BAG, limits)
    spread = (limits + 1) // 2
    counts = limits[None, :] - jax.random.randint(third, (EXAMPLES, TABLES), 0, BAG) % spread[None, :]
    chosen = jax.random.randint(fourth, (), 0, EXAMPLES)
    spot = (jnp.arange(EXAMPLES)[:, None] == chosen) & (columns[None, :] == busiest)
    counts = jnp.where(spot, BAG, counts)
    return counts.astype(jnp.int32)


def plant(drawn, stream_key, low, top_value):
    longest = drawn.shape.index(max(drawn.shape))
    spots = []
    for shift in (0, 1):
        where = [jax.random.randint(jax.random.fold_in(stream_key, axis), (), 0, length) for axis, length in enumerate(drawn.shape)]
        where[longest] = (where[longest] + shift) % drawn.shape[longest]
        spots.append(tuple(where))
    return drawn.at[spots[0]].set(low).at[spots[1]].set(top_value)


def steps_of(key, shape, shards, low, top_value):
    factor_of, own = 1.0, jax.random.fold_in(key, 6)
    for dim, parts in shards:
        draws = jnp.exp(jax.random.uniform(jax.random.fold_in(own, dim), (parts,), jnp.float32, low / len(shards), top_value / len(shards)))
        factor_of = factor_of * jnp.repeat(draws, shape[dim] // parts).reshape([-1 if axis == dim else 1 for axis in range(len(shape))])
    return factor_of


def rank_bounds(amount, lean):
    weights = [(1 << 20) // math.isqrt(rank ** lean) + 1 for rank in range(1, amount + 1)]
    deviation = 1 + sum(weights) // (1 << 30)
    return np.cumsum(np.array([max(1, weight // deviation) for weight in weights]))


def ranked(own_key, dims, amount, skew):
    listing = rank_bounds(amount, skew)
    lot = jax.random.randint(jax.random.fold_in(own_key, 1), dims, 0, int(listing[amount - 1]))
    standing = jnp.searchsorted(jnp.asarray(listing, jnp.int32), lot, side="right")
    return jax.random.permutation(jax.random.fold_in(own_key, 2), amount)[standing].astype(jnp.int32)


def gaussian(key, shape, width, most, pieces=(), kind=jnp.bfloat16):
    values = jax.random.normal(key, shape, jnp.float32) * width
    if len(pieces) > 0:
        values = steps_of(key, shape, pieces, -0.22, 0.18) * values
    return jnp.clip(values, min=-most, max=most).astype(kind)


def setup_inputs(seed: int = 0) -> dict:
    keys = jax.random.split(jax.random.key(seed), 5)
    return {
        "ids": plant(ranked(keys[0], (EXAMPLES, TABLES, BAG), ROWS, 2), jax.random.fold_in(keys[0], 3), 0, ROWS - 1).astype(jnp.int32),
        "lengths": draw_lengths(jax.random.fold_in(keys[4], 71), 0),
        "id_weights": jnp.clip(0.5 + 1.0 * jax.random.uniform(keys[2], (EXAMPLES, TABLES, BAG), jnp.float32) ** steps_of(keys[2], (EXAMPLES, TABLES, BAG), ((0, 32),), -0.2, 0.2), 0.5, 1.5),
        "table": gaussian(keys[3], (TABLES * ROWS, DIM), 0.3, 2.4, ((0, 32),), jnp.float32),
    }


def reference(ids, lengths, id_weights, table):
    slot = lax.broadcasted_iota(jnp.int32, ids.shape, 2)
    masked = jnp.where(slot < lengths[:, :, None], id_weights, jnp.zeros_like(id_weights))
    offsets = (jnp.arange(TABLES, dtype=jnp.int32) * ROWS).astype(jnp.int32)
    index = (ids + offsets[None, :, None]).astype(jnp.int32)
    index = jnp.transpose(index, (1, 0, 2)).reshape(TABLES, DEVICES, EX_DEV, BAG)
    weights = jnp.transpose(masked, (1, 0, 2)).reshape(TABLES, DEVICES, EX_DEV, BAG)

    def one_block(pair):
        rows = jnp.take(table, pair[0], axis=0)
        return jnp.sum(rows * pair[1][:, :, None], axis=1)

    def one_table(pair):
        return lax.map(one_block, pair)

    result = lax.map(one_table, (index, weights))
    result = result.reshape(TABLES, EXAMPLES, DIM)
    return jnp.transpose(result, (1, 0, 2))
```

```python
import functools

import jax
import jax.numpy as jnp
from jax import lax
from jax.experimental import pallas as pl
from jax.experimental.pallas import tpu as pltpu
from jax.sharding import PartitionSpec as P

AXES = ("group", "local")
LANES = 128
SUB = 8
ORDER = ((16, 2), (8, 2), (18, 2), (10, 2), (20, 4), (12, 4), (24, 4), (0, 4), (4, 4), (28, 4))
UNROLL = 4
VMEM_LIMIT = 16 * 1024 * 1024


def pack_kernel(k0, halves, me_ref, ids_ref, lengths_ref, w_ref, out_ref, *early):
    bag = ids_ref.shape[1]
    ids = ids_ref[...]
    row = (ids >> 3) * (SUB * halves) + (ids & (SUB - 1))
    out_ref[:, :bag, :] = row.astype(jnp.float32)
    slot = lax.broadcasted_iota(jnp.int32, ids.shape, 1)
    live = slot < lengths_ref[...][:, None, :]
    out_ref[:, bag:, :] = jnp.where(live, w_ref[...], 0.0)
    for n, ref in enumerate(early):
        ref[...] = out_ref[me_ref[0] ^ (k0 + n)]


def pack(me, k0, early, ids, lengths, w, halves):
    tables, bag, examples = ids.shape
    args = [pltpu.with_memory_space_constraint(x, pltpu.HBM) for x in (ids, lengths, w)]
    shapes = [(tables, 2 * bag, examples)] + [(2 * bag, examples)] * early
    return pl.pallas_call(
        functools.partial(pack_kernel, k0, halves),
        grid_spec=pltpu.PrefetchScalarGridSpec(
            num_scalar_prefetch=1,
            grid=(1,),
            in_specs=[pl.BlockSpec(x.shape, lambda i, m, n=x.ndim: (0,) * n) for x in args],
            out_specs=[pl.BlockSpec(x, lambda i, m, n=len(x): (0,) * n) for x in shapes],
        ),
        out_shape=[jax.ShapeDtypeStruct(x, jnp.float32) for x in shapes],
        compiler_params=pltpu.CompilerParams(vmem_limit_bytes=VMEM_LIMIT),
        name="pack",
    )(me, *args)


def lookup_kernel(k0, count, local, bag, unroll, halves, me_ref, idx_hbm, w_hbm, table_ref, prev_ref, *refs):
    *outs, idx, w_ref, buf, wt, acc, sems, w_sem = refs
    examples = w_ref.shape[2]
    words = bag * examples
    first = 0 if local else me_ref[0] ^ k0
    low = first % count
    start = pl.multiple_of((first - low) * words, words)
    copy = pltpu.make_async_copy(idx_hbm.at[pl.ds(start, count * words)], idx, sems.at[0])
    w_copy = pltpu.make_async_copy(w_hbm.at[pl.ds(first - low, count)], w_ref, w_sem)
    copy.start()
    w_copy.start()
    copy.wait()
    w_copy.wait()

    def block(b, carry):
        wt[...] = jnp.transpose(w_ref[low ^ b], (1, 0))
        here = (low ^ b) * words

        def group(g, carry):
            lead = g * (SUB * unroll)
            at = here + lead
            for u in range(unroll):
                for j in range(bag):
                    spots = [j * examples + u * SUB + k for k in range(SUB)]
                    rows = [idx.at[pl.ds(c, count * words - c)][at] for c in spots]
                    values = [table_ref[pl.ds(row, halves, stride=SUB), :] for row in rows]
                    for k, value in enumerate(values):
                        slot = ((u * bag + j) * SUB + k) * halves
                        buf[slot : slot + halves, :] = value
            for u in range(unroll):
                e = pl.multiple_of(lead + u * SUB, SUB)
                wv = wt[pl.ds(e, SUB), :]
                sums = [None] * halves
                for j in range(bag):
                    wj = jnp.broadcast_to(wv[:, j : j + 1], (SUB, LANES))
                    for h in range(halves):
                        slot = (u * bag + j) * SUB * halves + h
                        term = buf[pl.ds(slot, SUB, stride=halves), :] * wj
                        sums[h] = term if sums[h] is None else sums[h] + term
                for h in range(halves):
                    acc[pl.ds((b * examples + e) * halves + h, SUB, stride=halves), :] = sums[h]
            return carry

        return lax.fori_loop(0, examples // (SUB * unroll), group, carry)

    lax.fori_loop(0, count, block, 0)
    rows = acc.shape[0] // len(outs)
    copies = [
        pltpu.make_async_copy(acc.at[pl.ds(n * rows, rows), :], out, sems.at[n]) for n, out in enumerate(outs)
    ]
    for copy in copies:
        copy.start()
    for copy in copies:
        copy.wait()


def lookup(me, k0, count, idx, w, table, prev, halves, outs, local=False):
    _, bag, examples = w.shape
    unroll = UNROLL
    while examples % (unroll * SUB):
        unroll //= 2
    rows = count * halves * examples
    anywhere = pl.BlockSpec(memory_space=pl.ANY)
    out = pl.pallas_call(
        functools.partial(lookup_kernel, k0, count, local, bag, unroll, halves),
        in_specs=[
            pl.BlockSpec(memory_space=pltpu.SMEM),
            anywhere,
            anywhere,
            pl.BlockSpec(memory_space=pltpu.VMEM),
            anywhere,
        ],
        out_specs=[pl.BlockSpec(memory_space=pltpu.HBM)] * outs,
        out_shape=[pltpu.HBM((rows // outs, LANES), jnp.float32)] * outs,
        scratch_shapes=[
            pltpu.SMEM((count * bag * examples,), jnp.int32),
            pltpu.VMEM((count, bag, examples), jnp.float32),
            pltpu.VMEM((unroll * bag * halves * SUB, LANES), jnp.float32),
            pltpu.VMEM((examples, bag), jnp.float32),
            pltpu.VMEM((rows, LANES), jnp.float32),
            pltpu.SemaphoreType.DMA((outs,)),
            pltpu.SemaphoreType.DMA(()),
        ],
        compiler_params=pltpu.CompilerParams(vmem_limit_bytes=VMEM_LIMIT),
        name="lookup",
    )(me, idx, w, table, pltpu.with_memory_space_constraint(prev, pltpu.HBM))
    return list(out)


def place(me, k0, blocks, out, shape, halves):
    examples = shape[0]
    first = out is None
    steps = 2
    rows = halves * examples // steps
    args = [x for x, _ in blocks]
    specs = [pl.BlockSpec((rows, LANES), lambda s, m, n=n: (n * steps + s, 0)) for _, n in blocks]

    def kern(me_ref, *refs):
        out_ref = refs[-1]
        part = out_ref.shape[0]
        flat = out_ref.reshape(part * halves * SUB, LANES)
        for q in range(SUB):
            spot = ((me_ref[0] ^ k0) % SUB) ^ q
            flat[pl.ds(spot, part * halves, stride=SUB), :] = refs[q][...]

    return pl.pallas_call(
        kern,
        grid_spec=pltpu.PrefetchScalarGridSpec(
            num_scalar_prefetch=1,
            grid=(steps,),
            in_specs=specs + ([] if first else [pl.BlockSpec(memory_space=pl.ANY)]),
            out_specs=pl.BlockSpec((examples // steps, halves * SUB, LANES), lambda s, m: (s, (m[0] ^ k0) // SUB, 0)),
        ),
        out_shape=jax.ShapeDtypeStruct(shape, jnp.float32),
        input_output_aliases={} if first else {1 + SUB: 0},
        compiler_params=pltpu.CompilerParams(vmem_limit_bytes=VMEM_LIMIT),
        name="place",
    )(me, *args, *([] if first else [out]))


def second_halves(blocks, prev):
    rows = blocks[0].shape[0] // 2
    count = len(blocks)

    def kern(*refs):
        out_ref = refs[-1]
        for n in range(count):
            out_ref[pl.ds(n * rows, rows), :] = refs[n][...]

    return pl.pallas_call(
        kern,
        grid=(1,),
        in_specs=[pl.BlockSpec((rows, LANES), lambda i: (1, 0))] * count + [pl.BlockSpec(memory_space=pl.ANY)],
        out_specs=pl.BlockSpec((rows * count, LANES), lambda i: (0, 0)),
        out_shape=jax.ShapeDtypeStruct((rows * count, LANES), jnp.float32),
        compiler_params=pltpu.CompilerParams(vmem_limit_bytes=VMEM_LIMIT),
        name="halves",
    )(*blocks, pltpu.with_memory_space_constraint(prev, pltpu.HBM))


def plan(devices):
    unit = devices // 32
    return [(k * unit, count * unit) for k, count in ORDER]


def exchange(ids, lengths, id_weights, table):
    examples, tables, bag = ids.shape
    rows, width = table.shape
    devices = lax.axis_size("group") * lax.axis_size("local")
    halves = width // LANES
    me = (lax.axis_index("group") * lax.axis_size("local") + lax.axis_index("local")).reshape(1)

    view = table.reshape(rows // SUB, SUB, halves, LANES).transpose(0, 2, 1, 3).reshape(rows * halves, LANES)
    view = pltpu.with_memory_space_constraint(view, pltpu.VMEM)

    calls = plan(devices)
    lead, early = calls[0]
    packed, *ahead = pack(
        me, lead, early, jnp.transpose(ids, (1, 2, 0)), jnp.transpose(lengths), jnp.transpose(id_weights, (1, 2, 0)), halves)
    ahead = [lax.ppermute(x, AXES, [(i, i ^ (lead + n)) for i in range(devices)]) for n, x in enumerate(ahead)]
    arrived = lax.all_to_all(packed, AXES, split_axis=0, concat_axis=0, tiled=True)
    idx = arrived[:, :bag].astype(jnp.int32).reshape(-1)
    w = arrived[:, bag:]
    if early:
        ahead = jnp.stack(ahead)
        ahead_idx = ahead[:, :bag].astype(jnp.int32).reshape(-1)
        ahead_w = ahead[:, bag:]

    def swap(x, k):
        return lax.ppermute(x, AXES, [(i, i ^ k) for i in range(devices)])

    far = {}
    prev = packed
    last = calls[-1][0]
    direct = range(last, last + calls[-1][1])
    for n, (k, count) in enumerate(calls):
        size = 1 if k in direct else 2
        source = (ahead_idx, ahead_w) if n == 0 else (idx, w)
        pooled = lookup(me, k, count, *source, view, prev, halves, count // size, n == 0)
        prev = pooled[-1]
        for m, one in enumerate(pooled):
            at = k + m * size
            far[at] = swap(one, at) if at else one

    shape = (examples, tables * halves, LANES)
    out = None
    groups = sorted(range(0, devices, SUB), key=lambda g: max(n for n, (k, c) in enumerate(calls) if k < g + SUB and g < k + c))
    for g in groups:
        odd = [k for k in range(g, g + SUB, 2) if k not in direct]
        if odd:
            handed = swap(second_halves([far[k] for k in odd], prev), 1)
        blocks = []
        for k in range(g, g + SUB):
            if k in direct or k % 2 == 0:
                blocks.append((far[k], 0))
            else:
                blocks.append((handed, odd.index(k - 1)))
        out = place(me, g, blocks, out, shape, halves)
    out = out.reshape(examples, tables // SUB, halves, SUB, LANES)
    return out.transpose(0, 1, 3, 2, 4).reshape(examples, tables, width)


def solution(mesh):
    placed = (P(AXES, None, None), P(AXES, None), P(AXES, None, None), P(AXES, None))
    return jax.shard_map(exchange, mesh=mesh, in_specs=placed, out_specs=P(AXES, None, None), check_vma=False)
```
